32 devices in a mesh: dp: 1 (over z), tp: 32 (over y, x, core).
Axes of the slice: x: 4, y: 4, z: 1, core: 2. Of those that a mesh axis runs over, the one named last changes fastest.
The devices are a block of a 4x4x8 slice.
Arguments:
- x_seq: bfloat16 [1, 4096, 6144], P('dp', 'tp')
- ln_gain: float32 [6144], replicated
- ln_bias: float32 [6144], replicated
- w_qkv: bfloat16 [6144, 64, 3, 96], P(None, 'tp')
- w_out: bfloat16 [6144, 6144], P('tp')
- w_up: bfloat16 [6144, 24576], P(None, 'tp')
- w_down: bfloat16 [24576, 6144], P('tp')
Outputs:
- output: bfloat16 [1, 4096, 6144], P('dp', 'tp')
All inputs are finite; a program needn't handle non-finite values.
Results may differ from the reference program's by a relative error of at most 0.0126939.
Values are sent between devices in bfloat16 or wider.
A program may use at most 768 MiB of HBM per device.

```python
import jax
import jax.numpy as jnp
from jax import lax

D = 6144
HEADS = 64
KV_HEADS = 64
HEAD = 96
FF = 24576
BATCH = 1
SEQ = 4096

LN_EPS = 1e-5
GROUP_Q = HEADS // KV_HEADS


def normal_weights(key_w, shape, fan_in):
    return (jax.random.normal(key_w, shape, jnp.float32) * fan_in ** -0.5).astype(jnp.bfloat16)


def setup_inputs(seed: int = 0, part: int = 0) -> dict:
    root_key = jax.random.key(seed)
    key_x, key_c, key_g, key_b, key_qkv, key_o, key_up, key_dn = jax.random.split(root_key, 8)
    key_x = jax.random.fold_in(key_x, part)
    key_c = jax.random.fold_in(key_c, part)
    noise = jax.random.normal(key_x, (BATCH, SEQ, D), jnp.float32)
    shared = jax.random.normal(key_c, (BATCH, 1, D), jnp.float32)
    x_seq = ((noise + shared) * 0.7071).astype(jnp.bfloat16)
    ln_gain = 1.0 + 0.5 * jax.random.normal(key_g, (D,), jnp.float32)
    ln_bias = 0.5 * jax.random.normal(key_b, (D,), jnp.float32)
    w_qkv = normal_weights(key_qkv, (D, KV_HEADS, GROUP_Q + 2, HEAD), D)
    w_out = normal_weights(key_o, (HEADS * HEAD, D), HEADS * HEAD)
    w_up = normal_weights(key_up, (D, FF), D)
    w_down = normal_weights(key_dn, (FF, D), FF)
    return {"x_seq": x_seq, "ln_gain": ln_gain, "ln_bias": ln_bias, "w_qkv": w_qkv,
            "w_out": w_out, "w_up": w_up, "w_down": w_down}


def layer_norm(x_f32, ln_gain, ln_bias):
    row_mean = jnp.mean(x_f32, axis=-1, keepdims=True)
    centered = x_f32 - row_mean
    variance = jnp.mean(centered * centered, axis=-1, keepdims=True)
    return centered * lax.rsqrt(variance + LN_EPS) * ln_gain + ln_bias


def reference(x_seq, ln_gain, ln_bias, w_qkv, w_out, w_up, w_down):
    tokens = x_seq.reshape(BATCH * SEQ, D)
    normed = layer_norm(tokens.astype(jnp.float32), ln_gain, ln_bias).astype(jnp.bfloat16)
    proj_qkv = jnp.dot(normed, w_qkv.reshape(D, KV_HEADS * (GROUP_Q + 2) * HEAD),
                       preferred_element_type=jnp.float32).astype(jnp.bfloat16)
    proj_qkv = proj_qkv.reshape(BATCH, SEQ, KV_HEADS, GROUP_Q + 2, HEAD)
    proj_qkv = proj_qkv.transpose(0, 2, 3, 1, 4).reshape(BATCH * KV_HEADS, GROUP_Q + 2, SEQ, HEAD)
    causal = jnp.arange(SEQ)[:, None] >= jnp.arange(SEQ)[None, :]

    def one_group(group_item):
        query_rows = group_item[:GROUP_Q].astype(jnp.float32)
        key_rows = group_item[GROUP_Q].astype(jnp.float32)
        value_rows = group_item[GROUP_Q + 1].astype(jnp.float32)
        scores = jnp.einsum("jsh,th->jst", query_rows, key_rows) * (HEAD ** -0.5)
        scores = jnp.where(causal, scores, -jnp.inf)
        attn_prob = jax.nn.softmax(scores, axis=-1).astype(jnp.bfloat16)
        context = jnp.einsum("jst,th->jsh", attn_prob.astype(jnp.float32), value_rows)
        return context.astype(jnp.bfloat16)

    context = lax.map(one_group, proj_qkv)
    context = context.reshape(BATCH, KV_HEADS, GROUP_Q, SEQ, HEAD).transpose(0, 3, 1, 2, 4)
    context = context.reshape(BATCH * SEQ, HEADS * HEAD)
    attn_part = jnp.dot(context, w_out, preferred_element_type=jnp.float32)
    hidden = jnp.dot(normed, w_up, preferred_element_type=jnp.float32)
    activated = jax.nn.gelu(hidden, approximate=False).astype(jnp.bfloat16)
    mlp_part = jnp.dot(activated, w_down, preferred_element_type=jnp.float32)
    branch = (attn_part + mlp_part).astype(jnp.bfloat16)
    out_rows = (tokens.astype(jnp.float32) + branch.astype(jnp.float32)).astype(jnp.bfloat16)
    return out_rows.reshape(BATCH, SEQ, D)
```

```python
import functools

import jax
import jax.numpy as jnp
from jax import lax
from jax.experimental import pallas as pl
from jax.experimental.pallas import tpu as pltpu
from jax.sharding import PartitionSpec as P

OFFSETS = {"o": 0, "p": 1, "m": -1, "t": 2}


def decode(text, size):
    events = []
    for n in range(0, len(text), size):
        kind, i, j = text[n:n + 3]
        half = text[n + 3:n + size]
        events.append((kind, OFFSETS[i], OFFSETS[j]) + ((int(half),) if half.isdigit() else ()))
    return events


STEPS = [e[1:] for e in decode("-oo-op-om-po-mo-ot-to-pp-mp-pm-mm-pt-tp-mt-tm-tt", 3)]
BEFORE = [
    "aoo0aoo1loo-",
    "aop0aom0apo0amo0aop1aom1apo1amo1lop-lom-",
    "",
    "ato1",
    "",
    "lto-",
    "app1apm1",
    "lpp-",
    "amp1amm1lmp-",
    "atp0atm0lpm-lmm-",
    "atp1atm1",
    "apt0apt1lpt-",
    "ltp-amt0amt1lmt-",
    "ltm-",
    "att0att1",
    "ltt-",
]
BEFORE = [decode(text, 4) for text in BEFORE]
BETWEEN = [
    "",
    "lpo-",
    "apm0aot0ato0lmo-",
    "app0amm0",
    "aot1amp0lot-",
    "",
    "",
    "",
    "",
    "",
    "",
    "",
    "",
    "",
    "",
    "",
]
BETWEEN = [decode(text, 4) for text in BETWEEN]
EARLY = [e[1:] for e in decode("-oo-op-om-po-mo", 3)]
ORDER2 = [e[1:] for e in decode("-tt-tp-pt-tm-mt-pp-mm-pm-mp-ot-to-po-op-mo-om-oo", 3)]
EVENTS2 = [
    "",
    "",
    "Att",
    "Apt",
    "AtpLtp",
    "BtpAmt",
    "AtmLtm",
    "BtmAppLpp",
    "BppAmmLmm",
    "BmmAmpLmp",
    "BmpApmLpm",
    "BpmAtoLto",
    "BtoAot",
    "Aop",
    "Apo",
    "Aom",
    "LpoAmoLopBpoLmoBopAooBmoLomBomLooBoo",
]
EVENTS2 = [decode(text, 3) for text in EVENTS2]
NS = 10
MESH = pl.DeviceIdType.MESH
SIDE = 4
LN_EPS = 1e-5
f32, bf16 = jnp.float32, jnp.bfloat16
KT = 1024
CHUNKS = 3
NEG = -1e30
LOG2E = 1.4426950408889634


class Place:
    def __init__(self):
        self.tp = lax.axis_index("tp")
        self.colour = lax.rem(self.tp, 2)
        chip = lax.div(self.tp, 2)
        self.x, self.y = lax.rem(chip, SIDE), lax.div(chip, SIDE)

    def chip(self, colour, i, j):
        dx = (1 - colour) * i + colour * j
        dy = (1 - colour) * j + colour * i
        return lax.rem(self.y + dy + SIDE, SIDE) * SIDE + lax.rem(self.x + dx + SIDE, SIDE)

    def device(self, i, j):
        return {"tp": self.chip(self.colour, i, j) * 2 + self.colour}

    def partner(self):
        return {"tp": self.tp + 1 - 2 * self.colour}


def greet(place):
    barrier = pltpu.get_barrier_semaphore()
    others = [place.device(1, 0), place.device(-1, 0), place.device(0, 1), place.device(0, -1), place.partner()]
    for other in others:
        pl.semaphore_signal(barrier, inc=1, device_id=other, device_id_type=MESH)
    return lambda: pl.semaphore_wait(barrier, len(others))


def pick(step, values):
    r = jnp.int32(values[0])
    for n, v in enumerate(values[1:], 1):
        r = jnp.where(step == n, jnp.int32(v), r)
    return r


def layer_kernel(x_ref, gain_ref, bias_ref, wqkv_ref, wup_ref, wdown_ref, wout_ref,
                 y_ref, full_ref, act_ref, m_ref, m1_ref, m2_ref,
                 w, qq, kk, vv, lhs, dr, f1, f2, m_sc, l_sc, acc_sc,
                 recv, send, drecv, dsend, ssem, dssem, drsem, m1sem, m2sem, f1sem, f2sem, free, w_sem):
    place = Place()
    me = place.colour
    block, width = x_ref.shape
    half = block // 2
    ffl = wup_ref.shape[1]
    hd2 = wout_ref.shape[0]
    head = hd2 // 2
    pair = 2 * block
    n_steps = len(STEPS)
    ndr = dr.shape[0]
    cw = width // CHUNKS

    wloads = [pltpu.make_async_copy(wdown_ref, w.at[pl.ds(0, ffl)], w_sem.at[0]),
              pltpu.make_async_copy(wout_ref, w.at[pl.ds(ffl, hd2)], w_sem.at[1])]

    def rows_of(colour, i, j, h):
        first = (place.chip(colour, i, j) * 2 + colour) * block + h * half
        return full_ref.at[pl.ds(pl.multiple_of(first, half), half)]

    def chip_rows(ref, i, j):
        return ref.at[pl.ds(pl.multiple_of(place.chip(me, i, j) * pair, pair), pair)]

    def col_chunk(c):
        return pl.ds(pl.multiple_of(c * cw, cw), cw)

    sends = []

    def gather(xs, own, gain, bias, wqkv, wup, tile, acts, mst, in_sem, pw_sem, tile_sem, out_sem, mst_sem):
        loads = [pltpu.make_async_copy(x_ref, xs, in_sem.at[0]),
                 pltpu.make_async_copy(gain_ref, gain, in_sem.at[1]),
                 pltpu.make_async_copy(bias_ref, bias, in_sem.at[2])]
        pwloads = [pltpu.make_async_copy(wqkv_ref, wqkv, pw_sem.at[0]), pltpu.make_async_copy(wup_ref, wup, pw_sem.at[1])]
        for c in loads + pwloads + wloads:
            c.start()
        met = greet(place)
        for c in loads:
            c.wait()

        def norm_rows(start):
            g = gain[...]
            b = bias[...]

            @pl.loop(0, half // 16)
            def _(r):
                rows = pl.ds(pl.multiple_of(start + r * 16, 16), 16)
                v = xs[rows, :].astype(f32)
                mean = jnp.mean(v, axis=-1, keepdims=True)
                cen = v - mean
                var = jnp.mean(cen * cen, axis=-1, keepdims=True)
                own[rows, :] = (cen * lax.rsqrt(var + LN_EPS) * g + b).astype(bf16)

        def source(i, j, h):
            return own.at[pl.ds(h * half, half)] if (i, j) == (0, 0) else rows_of(me, i, j, h)

        def forward(i, j, h, to, ri, rj):
            n = len(sends)
            cp = pltpu.make_async_remote_copy(source(i, j, h), rows_of(me, i, j, h), send.at[n],
                                              recv.at[ri % SIDE, rj % SIDE, h], device_id=place.device(*to), device_id_type=MESH)
            cp.start()
            sends.append((i, j, h))

        def wait_block(colour, i, j, h, sem):
            r = rows_of(colour, i, j, h)
            pltpu.make_async_remote_copy(r, r, send.at[0], sem.at[i % SIDE, j % SIDE, h],
                                         device_id=place.partner(), device_id_type=MESH).wait_recv()

        def arrived(i, j, h):
            if (i, j) != (0, 0):
                wait_block(me, i, j, h, recv)
            if j == 0:
                if i == 0:
                    forward(0, 0, h, (-1, 0), 1, 0)
                    forward(0, 0, h, (1, 0), -1, 0)
                if (i, h) == (1, 0):
                    forward(i, 0, h, (-1, 0), 2, 0)
                if (i, h) == (-1, 1):
                    forward(i, 0, h, (1, 0), 2, 0)
                forward(i, j, h, (0, -1), i, 1)
                forward(i, j, h, (0, 1), i, -1)
            if (j, h) == (1, 0):
                forward(i, j, h, (0, -1), i, 2)
            if (j, h) == (-1, 1):
                forward(i, j, h, (0, 1), i, 2)
            pltpu.make_async_remote_copy(source(i, j, h), rows_of(me, i, j, h), dsend.at[i % SIDE, j % SIDE, h],
                                         drecv.at[i % SIDE, j % SIDE, h], device_id=place.partner(), device_id_type=MESH).start()

        def tile_load(s):
            i, j = STEPS[s]
            if s == 0:
                first = (place.chip(me, 0, 0) * 2 + 1 - me) * block
                return pltpu.make_async_copy(full_ref.at[pl.ds(pl.multiple_of(first, block), block)],
                                             tile.at[0, pl.ds(pl.multiple_of((1 - me) * block, block), block)], tile_sem.at[0])
            return pltpu.make_async_copy(chip_rows(full_ref, i, j), tile.at[s % 2], tile_sem.at[s % 2])

        def act_out(s):
            return pltpu.make_async_copy(acts.at[s % 2], chip_rows(act_ref, *STEPS[s]), out_sem.at[s % 2])

        def m_out(s):
            return [pltpu.make_async_copy(mst.at[c], chip_rows(m_ref, *STEPS[s]).at[:, pl.ds(c * cw, cw)], mst_sem.at[c])
                    for c in range(CHUNKS)]

        def serve(events):
            for e in events:
                if e[0] == "a":
                    arrived(*e[1:])
                else:
                    i, j = e[1:]
                    for h in range(2):
                        wait_block(1 - me, j, i, h, drecv)
                    tile_load(STEPS.index((i, j))).start()

        early = sorted(STEPS.index(c) for c in EARLY)
        norm_rows(0)
        met()
        serve([e for e in BEFORE[0] if e == ("a", 0, 0, 0)])
        norm_rows(half)
        serve([e for e in BEFORE[0] if e == ("a", 0, 0, 1)])
        tile[0, pl.ds(pl.multiple_of(me * block, block), block), :] = own[...]
        for g in range(2):
            qq[pl.ds(g * 128 + head, 128 - head), :] = jnp.zeros((128 - head, qq.shape[1]), bf16)

        @pl.loop(0, n_steps)
        def _(step):
            for s in range(n_steps):
                @pl.when(step == s)
                def _(s=s):
                    serve([e for e in BEFORE[s] if e[1:3] != (0, 0) or e[0] == "l"])
                    if s >= 2 and s - 2 not in early:
                        act_out(s - 2).wait()
                    if s == 0:
                        for c in pwloads:
                            c.wait()
                    tile_load(s).wait()

            p = lax.rem(step, 2)
            b = place.chip(me, pick(step, [i for i, _ in STEPS]), pick(step, [j for _, j in STEPS]))
            at = pl.ds(pl.multiple_of(b * pair, pair), pair)

            @pl.when(step >= 0)
            def _():
                n = tile[p]
                qkv = lax.dot_general(wqkv[...], n, (((1,), (1,)), ((), ())), preferred_element_type=f32)
                for g in range(2):
                    base = g * 3 * head
                    qq[pl.ds(g * 128, head), at] = qkv[base:base + head].astype(bf16)
                    keys = qkv[base + head:base + 2 * head]
                    keys = jnp.concatenate([keys, jnp.zeros((128 - head, pair), f32)], axis=0)
                    kk[at, pl.ds(g * 128, 128)] = keys.T.astype(bf16)
                    vv[pl.ds(g * head, head), at] = qkv[base + 2 * head:base + 3 * head].astype(bf16)
                hid = jnp.dot(n, wup[...], preferred_element_type=f32)
                acts[p] = (0.5 * hid * (1.0 + lax.erf(hid * (0.5 ** 0.5)))).astype(bf16)

            for s in range(n_steps):
                @pl.when(step == s)
                def _(s=s):
                    if s in early:
                        serve(BETWEEN[s])
                        if s == early[0]:
                            for c in wloads:
                                c.wait()
                        else:
                            for c in m_out(early[early.index(s) - 1]):
                                c.wait()
                    else:
                        act_out(s).start()

            if early:
                @pl.when(functools.reduce(jnp.logical_or, [step == s for s in early]))
                def _():
                    @pl.loop(0, CHUNKS)
                    def _(c):
                        mst[c] = jnp.dot(acts[p], w[0:ffl, col_chunk(c)], preferred_element_type=f32).astype(bf16)
                for s in early:
                    @pl.when(step == s)
                    def _(s=s):
                        for c in m_out(s):
                            c.start()

        for s in (n_steps - 2, n_steps - 1):
            if s not in early:
                act_out(s).wait()
        if early:
            for c in m_out(early[-1]):
                c.wait()
        else:
            for c in wloads:
                c.wait()
        for n, (i, j, h) in enumerate(sends):
            if (i, j) == (0, 0):
                pltpu.make_async_remote_copy(source(0, 0, h), rows_of(me, 0, 0, h), send.at[n], recv.at[0, 0, 0],
                                             device_id=place.partner(), device_id_type=MESH).wait_send()
        for h in range(2):
            pltpu.make_async_remote_copy(source(0, 0, h), rows_of(me, 0, 0, h), dsend.at[0, 0, h], recv.at[0, 0, 0],
                                         device_id=place.partner(), device_id_type=MESH).wait_send()

    pl.run_scoped(
        gather, pltpu.VMEM((block, width), bf16), pltpu.VMEM((block, width), bf16), pltpu.VMEM((1, width), f32), pltpu.VMEM((1, width), f32),
        pltpu.VMEM(wqkv_ref.shape, bf16), pltpu.VMEM(wup_ref.shape, bf16), pltpu.VMEM((2, pair, width), bf16),
        pltpu.VMEM((2, pair, ffl), bf16), pltpu.VMEM((CHUNKS, pair, cw), bf16),
        pltpu.SemaphoreType.DMA((3,)), pltpu.SemaphoreType.DMA((2,)), pltpu.SemaphoreType.DMA((2,)), pltpu.SemaphoreType.DMA((2,)),
        pltpu.SemaphoreType.DMA((CHUNKS,)))

    def scatter(xs, pool, stage, x_sem, lq_sem, st_sem):
        pltpu.make_async_copy(x_ref, xs, x_sem).start()

        def unit(s):
            return s % NS

        def hand_unit(s):
            return NS + s % (pool.shape[0] - NS)

        def step_loads(s):
            i, j = ORDER2[s]
            base = place.chip(me, i, j) * pair
            if (i, j) in EARLY:
                res = []
                for n, (colour, u) in enumerate(((me, unit(s)), (1 - me, hand_unit(s)))):
                    at = pl.ds(pl.multiple_of(base + colour * block, block), block)
                    res.append(pltpu.make_async_copy(m_ref.at[at], pool.at[u], lq_sem.at[s % 2, n]))
                return res
            return [pltpu.make_async_copy(chip_rows(act_ref, i, j), lhs.at[s % 2, :, pl.ds(0, ffl)], lq_sem.at[s % 2, 0])]

        def messages(i, j):
            if j == 2:
                return [(0, half, (0, 1), m1_ref.at[i % SIDE, 0], m1sem.at[i % SIDE, 0]),
                        (half, half, (0, -1), m1_ref.at[i % SIDE, 1], m1sem.at[i % SIDE, 1])]
            if j == 1:
                return [(0, block, (0, 1), m2_ref.at[i % SIDE, 0], m2sem.at[i % SIDE, 0])]
            if j == -1:
                return [(0, block, (0, -1), m2_ref.at[i % SIDE, 1], m2sem.at[i % SIDE, 1])]
            if i == 2:
                return [(0, half, (1, 0), f1.at[0], f1sem.at[0]), (half, half, (-1, 0), f1.at[1], f1sem.at[1])]
            if i == 1:
                return [(0, block, (1, 0), f2.at[0], f2sem.at[0])]
            if i == -1:
                return [(0, block, (-1, 0), f2.at[1], f2sem.at[1])]
            return []

        def copies(i, j):
            s = ORDER2.index((i, j))
            return [pltpu.make_async_remote_copy(pool.at[unit(s), pl.ds(r, n)], ref, ssem.at[s, m], sem,
                                                 device_id=place.device(*to), device_id_type=MESH)
                    for m, (r, n, to, ref, sem) in enumerate(messages(i, j))]

        def wait_in(ref, sem):
            pltpu.make_async_remote_copy(ref, ref, ssem.at[0, 0], sem, device_id=place.partner(), device_id_type=MESH).wait_recv()

        def hand_over(s):
            return [pltpu.make_async_remote_copy(pool.at[hand_unit(s), :, pl.ds(c * cw, cw)], dr.at[s % ndr, :, pl.ds(c * cw, cw)],
                                                 dssem.at[s % 4, c], drsem.at[s, c],
                                                 device_id=place.partner(), device_id_type=MESH) for c in range(CHUNKS)]

        def stage_a(i, j):
            u = unit(ORDER2.index((i, j)))
            msg = ORDER2.index((j, i))
            for c in hand_over(msg):
                c.wait_recv()

            @pl.loop(0, block // 16)
            def _(r):
                rows = pl.ds(pl.multiple_of(r * 16, 16), 16)
                pool[u, rows, :] = (pool[u, rows, :].astype(f32) + dr[msg % ndr, rows, :].astype(f32)).astype(bf16)

            if msg + ndr < n_steps:
                pl.semaphore_signal(free.at[msg % ndr], inc=1, device_id=place.partner(), device_id_type=MESH)
            if j == 2:
                for c in copies(i, j):
                    c.start()

        def staged(i, j, p):
            if j == 0:
                return [pltpu.make_async_copy(m2_ref.at[i % SIDE, d], stage.at[p, d], st_sem.at[p, d]) for d in range(2)]
            d = 0 if j == 1 else 1
            return [pltpu.make_async_copy(m1_ref.at[i % SIDE, d], stage.at[p, 0, pl.ds(0, half)], st_sem.at[p, 0])]

        turn = {}

        def load_in(i, j):
            turn[(i, j)] = len(turn) % 2
            if j == 0:
                for d in range(2):
                    wait_in(m2_ref.at[i % SIDE, d], m2sem.at[i % SIDE, d])
            else:
                d = 0 if j == 1 else 1
                wait_in(m1_ref.at[i % SIDE, d], m1sem.at[i % SIDE, d])
            for c in staged(i, j, turn[(i, j)]):
                c.start()
            if j == 0 and i in (1, -1):
                d = 0 if i == 1 else 1
                wait_in(f1.at[d], f1sem.at[d])
            if j == 0 and i == 0:
                for d in range(2):
                    wait_in(f2.at[d], f2sem.at[d])

        def stage_b(i, j):
            p = turn[(i, j)]
            u = unit(ORDER2.index((i, j)))
            for c in staged(i, j, p):
                c.wait()
            if (i, j) == (0, 0):
                pltpu.make_async_copy(x_ref, xs, x_sem).wait()
            for h in range(2):
                if (j, h) in ((1, 1), (-1, 0)):
                    continue

                @pl.loop(0, half // 16)
                def _(r, h=h):
                    rows = pl.ds(pl.multiple_of(h * half + r * 16, 16), 16)
                    near = pl.ds(pl.multiple_of(r * 16, 16), 16)
                    total = pool[u, rows, :].astype(f32)
                    if j != 0:
                        total = total + stage[p, 0, near, :].astype(f32)
                    else:
                        total = total + stage[p, 0, rows, :].astype(f32) + stage[p, 1, rows, :].astype(f32)
                        if (i, h) == (1, 0):
                            total = total + f1[0, near, :].astype(f32)
                        if (i, h) == (-1, 1):
                            total = total + f1[1, near, :].astype(f32)
                        if i == 0:
                            total = total + f2[0, rows, :].astype(f32) + f2[1, rows, :].astype(f32)
                            total = xs[rows, :].astype(f32) + total.astype(bf16).astype(f32)
                    pool[u, rows, :] = total.astype(bf16)
            for c in copies(i, j):
                c.start()

        def serve(events):
            for kind, i, j in events:
                {"A": stage_a, "L": load_in, "B": stage_b}[kind](i, j)

        for c in step_loads(0):
            c.start()

        @pl.loop(0, n_steps)
        def _(step):
            for s in range(n_steps):
                @pl.when(step == s)
                def _(s=s):
                    serve(EVENTS2[s])
                    for c in step_loads(s):
                        c.wait()
                    if s + 1 < n_steps:
                        if s + 1 >= NS:
                            for c in copies(*ORDER2[s + 1 - NS]):
                                c.wait_send()
                        if s + 1 >= pool.shape[0] - NS:
                            for c in hand_over(s + 1 - (pool.shape[0] - NS)):
                                c.wait_send()
                        for c in step_loads(s + 1):
                            c.start()

            p = lax.rem(step, 2)
            b = place.chip(me, pick(step, [i for i, _ in ORDER2]), pick(step, [j for _, j in ORDER2]))
            scale = head ** -0.5 * LOG2E

            @pl.when(step >= 0)
            def _():
                m_sc[...] = jnp.full(m_sc.shape, NEG, f32)
                l_sc[...] = jnp.zeros(l_sc.shape, f32)
                acc_sc[...] = jnp.zeros(acc_sc.shape, f32)

            q_at = pl.ds(pl.multiple_of(b * pair, pair), pair)

            def attend(t, masked):
                rows = pl.ds(pl.multiple_of(t * KT, KT), KT)
                scores = []
                for g in range(2):
                    sc = jnp.dot(kk[rows, g * 128:(g + 1) * 128], qq[g * 128:(g + 1) * 128, q_at], preferred_element_type=f32)
                    if masked:
                        kp = t * KT + lax.broadcasted_iota(jnp.int32, (KT, pair), 0)
                        qp = b * pair + lax.broadcasted_iota(jnp.int32, (KT, pair), 1)
                        sc = jnp.where(kp <= qp, sc, NEG)
                    scores.append(sc)
                for g in range(2):
                    sc = scores[g]
                    old = m_sc[g:g + 1, :]
                    top = jnp.maximum(old, jnp.max(sc, axis=0, keepdims=True))
                    keep = jnp.exp2((old - top) * scale)
                    pr = jnp.exp2((sc - top) * scale)
                    l_sc[g:g + 1, :] = l_sc[g:g + 1, :] * keep + jnp.sum(pr, axis=0, keepdims=True)
                    acc_sc[g] = acc_sc[g] * keep + jnp.dot(vv[g * head:(g + 1) * head, rows], pr.astype(bf16),
                                                           preferred_element_type=f32)
                    m_sc[g:g + 1, :] = top

            full = lax.div(b, KT // pair)

            @pl.loop(0, full)
            def _(t):
                attend(t, False)

            @pl.when(step >= 0)
            def _():
                attend(full, True)
                for g in range(2):
                    o = acc_sc[g] / l_sc[g:g + 1, :]
                    lhs[p, :, pl.ds(ffl + g * head, head)] = o.T.astype(bf16)

            mine, theirs = lax.rem(step, NS), NS + lax.rem(step, pool.shape[0] - NS)
            low = mine * (1 - me) + theirs * me
            high = mine * me + theirs * (1 - me)
            is_early = functools.reduce(jnp.logical_or, [step == ORDER2.index(c) for c in EARLY]) if EARLY else step < 0

            @pl.when(is_early)
            def _():
                @pl.loop(0, CHUNKS)
                def _(c):
                    cols = col_chunk(c)
                    r = jnp.dot(lhs[p, :, ffl:ffl + hd2], w[ffl:ffl + hd2, cols], preferred_element_type=f32)
                    pool[low, :, cols] = (pool[low, :, cols].astype(f32) + r[:block]).astype(bf16)
                    pool[high, :, cols] = (pool[high, :, cols].astype(f32) + r[block:]).astype(bf16)

            @pl.when(jnp.logical_not(is_early))
            def _():
                @pl.loop(0, CHUNKS)
                def _(c):
                    cols = col_chunk(c)
                    r = jnp.dot(lhs[p, :, 0:ffl + hd2], w[:, cols], preferred_element_type=f32)
                    pool[low, :, cols] = r[:block].astype(bf16)
                    pool[high, :, cols] = r[block:].astype(bf16)

            for s in range(n_steps):
                @pl.when(step == s)
                def _(s=s):
                    if s >= ndr:
                        pl.semaphore_wait(free.at[s % ndr], 1)
                    for c in hand_over(s):
                        c.start()

        serve(EVENTS2[n_steps])
        out = pltpu.make_async_copy(pool.at[unit(ORDER2.index((0, 0)))], y_ref, x_sem)
        out.start()
        for s in range(n_steps - NS, n_steps):
            for c in copies(*ORDER2[s]):
                c.wait_send()
        for s in range(n_steps - (pool.shape[0] - NS), n_steps):
            for c in hand_over(s):
                c.wait_send()
        out.wait()

    pl.run_scoped(scatter, pltpu.VMEM((block, width), bf16), pltpu.VMEM((NS + 3, block, width), bf16),
                  pltpu.VMEM((2, 2, block, width), bf16),
                  pltpu.SemaphoreType.DMA, pltpu.SemaphoreType.DMA((2, 2)), pltpu.SemaphoreType.DMA((2, 2)))

    for n, (i, j, h) in enumerate(sends):
        if (i, j) != (0, 0):
            r = rows_of(me, i, j, h)
            pltpu.make_async_remote_copy(r, r, send.at[n], recv.at[0, 0, 0], device_id=place.partner(), device_id_type=MESH).wait_send()
    for i, j in STEPS[1:]:
        for h in range(2):
            r = rows_of(me, i, j, h)
            pltpu.make_async_remote_copy(r, r, dsend.at[i % SIDE, j % SIDE, h], recv.at[0, 0, 0],
                                         device_id=place.partner(), device_id_type=MESH).wait_send()


def layer(x, gain, bias, w_qkv, w_up, w_down, w_out, n_tp):
    block, width = x.shape
    seq = n_tp * block
    d, groups, three, head = w_qkv.shape
    wq = w_qkv.transpose(1, 2, 3, 0).reshape(groups * three * head, d)
    ffl = w_up.shape[1]
    hd2 = groups * head
    half = block // 2
    hbm = pl.BlockSpec(memory_space=pltpu.HBM)
    V, D, S = pltpu.VMEM, pltpu.SemaphoreType.DMA, jax.ShapeDtypeStruct
    return pl.pallas_call(
        layer_kernel,
        out_shape=(S((block, width), bf16), S((seq, width), bf16), S((seq, ffl), bf16), S((seq, width), bf16),
                   S((SIDE, 2, half, width), bf16), S((SIDE, 2, block, width), bf16)),
        in_specs=[hbm] * 7, out_specs=(hbm,) * 6,
        scratch_shapes=[
            V((ffl + hd2, width), bf16), V((groups * 128, seq), bf16), V((seq, groups * 128), bf16), V((hd2, seq), bf16),
            V((2, 2 * block, -(-(ffl + hd2) // 128) * 128), bf16), V((4, block, width), bf16),
            V((2, half, width), bf16), V((2, block, width), bf16),
            V((8, 2 * block), f32), V((8, 2 * block), f32), V((groups, head, 2 * block), f32),
            D((SIDE, SIDE, 2)), D((30,)), D((SIDE, SIDE, 2)), D((SIDE, SIDE, 2)),
            D((16, 2)), D((4, CHUNKS)), D((16, CHUNKS)), D((SIDE, 2)), D((SIDE, 2)), D((2,)), D((2,)),
            pltpu.SemaphoreType.REGULAR((4,)), D((2,))],
        compiler_params=pltpu.CompilerParams(collective_id=0, has_side_effects=True, vmem_limit_bytes=67043328),
        name="parallel_layer",
    )(x, gain.reshape(1, -1), bias.reshape(1, -1), wq, w_up, w_down, w_out)[0]


def solution(mesh):
    n_tp = mesh.shape["tp"]
    assert n_tp == 2 * SIDE * SIDE

    def local_layer(x_blk, ln_gain, ln_bias, w_qkv, w_out, w_up, w_down):
        x = x_blk.reshape(x_blk.shape[1:])
        return layer(x, ln_gain, ln_bias, w_qkv, w_up, w_down, w_out, n_tp)[None]

    return jax.shard_map(
        local_layer, mesh=mesh,
        in_specs=(P("dp", "tp", None), P(), P(), P(None, "tp", None, None),
                  P("tp", None), P(None, "tp"), P("tp", None)),
        out_specs=P("dp", "tp", None), check_vma=False)
```

```python
import functools

import jax
import jax.numpy as jnp
from jax import lax
from jax.experimental import pallas as pl
from jax.experimental.pallas import tpu as pltpu
from jax.sharding import PartitionSpec as P

OFFSETS = {"o": 0, "p": 1, "m": -1, "t": 2}


def place_of(text):
    return OFFSETS[text[0]], OFFSETS[text[1]]


def split(text, size):
    return [text[n:n + size] for n in range(0, len(text), size)]


def gather_events(text):
    return [("l", int(e[1:3])) if e[0] == "l" else (e[0],) + place_of(e[1:]) + (int(e[3]),) for e in split(text, 4)]


def scatter_events(text):
    return [(e[0],) + place_of(e[1:]) for e in split(text, 3)]


TILES = [
    "oo0oo1",
    "op0om1",
    "po0mo1",
    "op1om0",
    "po1mo0",
    "pp0mm1",
    "ot0ot1",
    "to0to1",
    "pm1mp0",
    "pm0mp1",
    "pt0mt1",
    "tp0tm1",
    "pt1mt0",
    "tp1tm0",
    "tt0tt1",
    "pp1mm0",
]
TILES = [[(place_of(u), int(u[2])) for u in split(text, 3)] for text in TILES]
BEFORE = [
    "aoo0aoo1Eoo1Eoo0Woo0Woo1Uoo1Uoo0Doo0Doo1l00-",
    "aop0aom1apo0amo1Emo1Wpo0Umo1Uom1Dpo0Dop0l01-l02-",
    "",
    "Upo0Dmo1aop1aom0apo1amo0l03-l04-",
    "",
    "Upo1Dmo0app0amm1ato0ato1l05-",
    "aot0aot1Uto1Dto0l06-",
    "apm0amp1",
    "apm1amp0l08-",
    "Upm1Dmp0l09-atp0atm1",
    "Utm1Dtp0apt0amt1l10-",
    "atp1atm0",
    "apt1amt0l12-",
    "att0att1",
    "",
    "l15-",
]
BEFORE = [gather_events(text) for text in BEFORE]
BETWEEN = [
    "",
    "",
    "",
    "",
    "",
    "",
    "Umm1Dpp0l07-",
    "Uto0Dto1",
    "",
    "",
    "Umo0Dpo1l11-",
    "",
    "l13-",
    "l14-",
    "app1amm0",
    "",
]
BETWEEN = [gather_events(text) for text in BETWEEN]
DOWNS = [0, 6, 7, 10, 11, 12, 13, 14]
EARLY = [place_of(text) for text in split("oootptmttotptmtt", 2)]
ORDER2 = [place_of(text) for text in split("tttppttmmtppmmpmmpottopoopmoomoo", 2)]
EVENTS2 = [
    "",
    "",
    "",
    "Apt",
    "Ltp",
    "Amt",
    "Btm",
    "Bpp",
    "Bmm",
    "AmpLmp",
    "Bpm",
    "AtoLto",
    "",
    "Aop",
    "",
    "Aom",
    "BpoBmoAooLomLopBomBopLooBoo",
]
EVENTS2 = [scatter_events(text) for text in EVENTS2]
MIDDLE2 = [
    "",
    "Att",
    "",
    "Atp",
    "Btp",
    "AtmLtm",
    "AppLpp",
    "AmmLmm",
    "",
    "BmpApmLpm",
    "",
    "BtoAot",
    "",
    "Apo",
    "",
    "LpoAmoLmo",
]
MIDDLE2 = [scatter_events(text) for text in MIDDLE2]
NS = 11
MESH = pl.DeviceIdType.MESH
SIDE = 4
LN_EPS = 1e-5
f32, bf16 = jnp.float32, jnp.bfloat16
KT = 1024
CHUNKS = 3
FINAL_STEPS = 2
NEG = -1e30
LOG2E = 1.4426950408889634


class Place:
    def __init__(self):
        self.tp = lax.axis_index("tp")
        self.colour = lax.rem(self.tp, 2)
        chip = lax.div(self.tp, 2)
        self.x, self.y = lax.rem(chip, SIDE), lax.div(chip, SIDE)

    def chip(self, colour, i, j):
        dx = (1 - colour) * i + colour * j
        dy = (1 - colour) * j + colour * i
        return lax.rem(self.y + dy + SIDE, SIDE) * SIDE + lax.rem(self.x + dx + SIDE, SIDE)

    def device(self, i, j):
        return {"tp": self.chip(self.colour, i, j) * 2 + self.colour}

    def partner(self):
        return {"tp": self.tp + 1 - 2 * self.colour}


def greet(place):
    barrier = pltpu.get_barrier_semaphore()
    others = [place.device(1, 0), place.device(-1, 0), place.device(0, 1), place.device(0, -1), place.partner()]
    for other in others:
        pl.semaphore_signal(barrier, inc=1, device_id=other, device_id_type=MESH)
    return lambda: pl.semaphore_wait(barrier, len(others))


ROUTES = {"W": (-1, 0), "E": (1, 0), "D": (0, -1), "U": (0, 1)}


def at_steps(step, count, body):
    for first in range(0, count, 4):
        @pl.when(jnp.logical_and(step >= first, step < first + 4))
        def _(first=first):
            for s in range(first, min(first + 4, count)):
                @pl.when(step == s)
                def _(s=s):
                    body(s)


def pick(step, values):
    r = jnp.int32(values[0])
    for n, v in enumerate(values[1:], 1):
        r = jnp.where(step == n, jnp.int32(v), r)
    return r


def layer_kernel(x_ref, gain_ref, bias_ref, wqkv_ref, wup_ref, wdown_ref, wout_ref,
                 p_ref, full_ref, act_ref, m_ref, m1_ref, m2_ref, f2,
                 w, qq, kk, vv, lhs, dr, f1, m_sc, l_sc, acc_sc,
                 recv, send, drecv, dsend, ssem, dssem, drsem, m1sem, m2sem, f1sem, f2sem, free, w_sem):
    place = Place()
    me = place.colour
    block, width = x_ref.shape
    half = block // 2
    ffl = wup_ref.shape[1]
    hd2 = wout_ref.shape[0]
    head = hd2 // 2
    pair = 2 * block
    n_steps = len(TILES)
    ndr = dr.shape[0]
    cw = width // CHUNKS

    wloads = [pltpu.make_async_copy(wdown_ref, w.at[pl.ds(0, ffl)], w_sem.at[0]),
              pltpu.make_async_copy(wout_ref, w.at[pl.ds(ffl, hd2)], w_sem.at[1])]

    def rows_of(colour, i, j, h):
        first = (place.chip(colour, i, j) * 2 + colour) * block + h * half
        return full_ref.at[pl.ds(pl.multiple_of(first, half), half)]

    def chip_rows(ref, i, j):
        return ref.at[pl.ds(pl.multiple_of(place.chip(me, i, j) * pair, pair), pair)]

    sent = [e for t in range(n_steps) for e in BEFORE[t] + BETWEEN[t] if e[0] in ROUTES]

    def stored(unit):
        (i, j), h = unit
        return pl.ds(pl.multiple_of(place.chip(me, i, j) * pair + h * block, block), block)

    def gather(xs, own, gain, bias, wqkv, wup, tile, acts, mst, in_sem, pw_sem, tile_sem, out_sem, mst_sem):
        loads = [pltpu.make_async_copy(x_ref, xs, in_sem.at[0]),
                 pltpu.make_async_copy(gain_ref, gain, in_sem.at[1]),
                 pltpu.make_async_copy(bias_ref, bias, in_sem.at[2])]
        pwloads = [pltpu.make_async_copy(wqkv_ref, wqkv, pw_sem.at[0]), pltpu.make_async_copy(wup_ref, wup, pw_sem.at[1])]
        for c in loads + pwloads + wloads:
            c.start()
        met = greet(place)
        for c in loads:
            c.wait()

        def norm_rows(start):
            g = gain[...]
            b = bias[...]

            @pl.loop(0, half // 16)
            def _(r):
                rows = pl.ds(pl.multiple_of(start + r * 16, 16), 16)
                v = xs[rows, :].astype(f32)
                mean = jnp.mean(v, axis=-1, keepdims=True)
                cen = v - mean
                var = jnp.mean(cen * cen, axis=-1, keepdims=True)
                own[rows, :] = (cen * lax.rsqrt(var + LN_EPS) * g + b).astype(bf16)

        def source(i, j, h):
            return own.at[pl.ds(h * half, half)] if (i, j) == (0, 0) else rows_of(me, i, j, h)

        def forward(kind, i, j, h):
            di, dj = ROUTES[kind]
            ri, rj = (i - di) % SIDE, (j - dj) % SIDE
            pltpu.make_async_remote_copy(source(i, j, h), rows_of(me, i, j, h), send.at[sent.index((kind, i, j, h))],
                                         recv.at[ri, rj, h], device_id=place.device(di, dj), device_id_type=MESH).start()

        def wait_block(colour, i, j, h, sem):
            r = rows_of(colour, i, j, h)
            pltpu.make_async_remote_copy(r, r, send.at[0], sem.at[i % SIDE, j % SIDE, h],
                                         device_id=place.partner(), device_id_type=MESH).wait_recv()

        def arrived(i, j, h):
            if (i, j) != (0, 0):
                wait_block(me, i, j, h, recv)
            pltpu.make_async_remote_copy(source(i, j, h), rows_of(me, i, j, h), dsend.at[i % SIDE, j % SIDE, h],
                                         drecv.at[i % SIDE, j % SIDE, h], device_id=place.partner(), device_id_type=MESH).start()

        def tile_parts(t, load):
            parts = []
            for u, ((i, j), h) in enumerate(TILES[t]):
                for n, colour in enumerate((me, 1 - me)):
                    if (i, j) == (0, 0) and n == 0:
                        if load:
                            tile[t % 2, pl.ds(pl.multiple_of(u * block + colour * half, half), half), :] = own[pl.ds(h * half, half), :]
                        continue
                    if load and n == 1:
                        wait_block(colour, j, i, h, drecv)
                    src = rows_of(me, i, j, h) if n == 0 else rows_of(colour, j, i, h)
                    parts.append(pltpu.make_async_copy(
                        src, tile.at[t % 2, pl.ds(pl.multiple_of(u * block + colour * half, half), half)],
                        tile_sem.at[t % 2, 2 * u + n]))
            return parts

        def act_out(t):
            return [pltpu.make_async_copy(acts.at[t % 2, pl.ds(u * block, block)], act_ref.at[stored(unit)], out_sem.at[t % 2, u])
                    for u, unit in enumerate(TILES[t]) if unit[0] not in EARLY]

        def m_out(t):
            return [pltpu.make_async_copy(mst.at[c, pl.ds(u * block, block)],
                                          m_ref.at[stored(unit), pl.ds(c * cw, cw)], mst_sem.at[c, u])
                    for c in range(CHUNKS) for u, unit in enumerate(TILES[t]) if unit[0] in EARLY]

        def serve(events):
            for e in events:
                if e[0] == "a":
                    arrived(*e[1:])
                elif e[0] == "l":
                    for c in tile_parts(e[1], True):
                        c.start()
                else:
                    forward(*e)

        norm_rows(0)
        norm_rows(half)
        met()
        serve([e for e in BEFORE[0] if e[0] != "l"])
        for g in range(2):
            qq[pl.ds(g * 128 + head, 128 - head), :] = jnp.zeros((128 - head, qq.shape[1]), bf16)

        @pl.loop(0, n_steps)
        def _(step):
            @functools.partial(at_steps, step, n_steps)
            def _(s):
                serve([e for e in BEFORE[s] if s or e[0] == "l"])
                if s >= 2:
                    for c in act_out(s - 2):
                        c.wait()
                if s == 0:
                    for c in pwloads:
                        c.wait()
                for c in tile_parts(s, False):
                    c.wait()

            p = lax.rem(step, 2)
            homes = []
            for u in range(2):
                units = [t[u] for t in TILES]
                b = place.chip(me, pick(step, [i for (i, _), _ in units]), pick(step, [j for (_, j), _ in units]))
                homes.append(pl.ds(pl.multiple_of(b * pair + pick(step, [h for _, h in units]) * block, block), block))

            @pl.when(step >= 0)
            def _():
                n = tile[p]
                qkv = lax.dot_general(wqkv[...], n, (((1,), (1,)), ((), ())), preferred_element_type=f32)
                for g in range(2):
                    base = g * 3 * head
                    keys = qkv[base + head:base + 2 * head]
                    keys = jnp.concatenate([keys, jnp.zeros((128 - head, pair), f32)], axis=0).T.astype(bf16)
                    for u in range(2):
                        cols = slice(u * block, (u + 1) * block)
                        qq[pl.ds(g * 128, head), homes[u]] = qkv[base:base + head, cols].astype(bf16)
                        kk[homes[u], pl.ds(g * 128, 128)] = keys[cols]
                        vv[pl.ds(g * head, head), homes[u]] = qkv[base + 2 * head:base + 3 * head, cols].astype(bf16)
                hid = jnp.dot(n, wup[...], preferred_element_type=f32)
                acts[p] = (0.5 * hid * (1.0 + lax.erf(hid * (0.5 ** 0.5)))).astype(bf16)

            @functools.partial(at_steps, step, n_steps)
            def _(s):
                serve(BETWEEN[s])
                for c in act_out(s):
                    c.start()
                if s in DOWNS:
                    if s == DOWNS[0]:
                        for c in wloads:
                            c.wait()
                    else:
                        for c in m_out(DOWNS[DOWNS.index(s) - 1]):
                            c.wait()

            @pl.when(functools.reduce(jnp.logical_or, [step == s for s in DOWNS]))
            def _():
                for c in range(CHUNKS):
                    mst[c] = jnp.dot(acts[p], w[0:ffl, c * cw:(c + 1) * cw], preferred_element_type=f32).astype(bf16)

            @functools.partial(at_steps, step, n_steps)
            def _(s):
                if s in DOWNS:
                    for c in m_out(s):
                        c.start()

        for s in (n_steps - 2, n_steps - 1):
            for c in act_out(s):
                c.wait()
        for c in m_out(DOWNS[-1]):
            c.wait()
        for n, (_, i, j, h) in enumerate(sent):
            if (i, j) == (0, 0):
                pltpu.make_async_remote_copy(source(0, 0, h), rows_of(me, 0, 0, h), send.at[n], recv.at[0, 0, 0],
                                             device_id=place.partner(), device_id_type=MESH).wait_send()
        for h in range(2):
            pltpu.make_async_remote_copy(source(0, 0, h), rows_of(me, 0, 0, h), dsend.at[0, 0, h], recv.at[0, 0, 0],
                                         device_id=place.partner(), device_id_type=MESH).wait_send()

    pl.run_scoped(
        gather, pltpu.VMEM((block, width), bf16), pltpu.VMEM((block, width), bf16), pltpu.VMEM((1, width), f32), pltpu.VMEM((1, width), f32),
        pltpu.VMEM(wqkv_ref.shape, bf16), pltpu.VMEM(wup_ref.shape, bf16), pltpu.VMEM((2, pair, width), bf16),
        pltpu.VMEM((2, pair, ffl), bf16), pltpu.VMEM((CHUNKS, pair, cw), bf16),
        pltpu.SemaphoreType.DMA((3,)), pltpu.SemaphoreType.DMA((2,)), pltpu.SemaphoreType.DMA((2, 4)), pltpu.SemaphoreType.DMA((2, 2)),
        pltpu.SemaphoreType.DMA((CHUNKS, 2)))

    def scatter(pool, stage, out_sem, lq_sem, st_sem):

        def unit(s):
            return s % NS

        def hand_unit(s):
            return NS + s % (pool.shape[0] - NS)

        def step_loads(s):
            i, j = ORDER2[s]
            base = place.chip(me, i, j) * pair
            if (i, j) in EARLY:
                res = []
                for n, (colour, u) in enumerate(((me, unit(s)), (1 - me, hand_unit(s)))):
                    for h in range(2):
                        at = pl.ds(pl.multiple_of(base + h * block + colour * half, half), half)
                        res.append(pltpu.make_async_copy(m_ref.at[at], pool.at[u, pl.ds(h * half, half)], lq_sem.at[s % 2, 2 * n + h]))
                return res
            return [pltpu.make_async_copy(chip_rows(act_ref, i, j), lhs.at[s % 2, :, pl.ds(0, ffl)], lq_sem.at[s % 2, 0])]

        def messages(i, j):
            if j == 2:
                return [(0, half, (0, 1), m1_ref.at[i % SIDE, 0], m1sem.at[i % SIDE, 0]),
                        (half, half, (0, -1), m1_ref.at[i % SIDE, 1], m1sem.at[i % SIDE, 1])]
            if j == 1:
                return [(0, block, (0, 1), m2_ref.at[i % SIDE, 0], m2sem.at[i % SIDE, 0])]
            if j == -1:
                return [(0, block, (0, -1), m2_ref.at[i % SIDE, 1], m2sem.at[i % SIDE, 1])]
            if i == 2:
                return [(0, half, (1, 0), f1.at[0], f1sem.at[0]), (half, half, (-1, 0), f1.at[1], f1sem.at[1])]
            if i == 1:
                return [(0, block, (1, 0), f2.at[0], f2sem.at[0])]
            if i == -1:
                return [(0, block, (-1, 0), f2.at[1], f2sem.at[1])]
            return []

        def copies(i, j):
            s = ORDER2.index((i, j))
            return [pltpu.make_async_remote_copy(pool.at[unit(s), pl.ds(r, n)], ref, ssem.at[s, m], sem,
                                                 device_id=place.device(*to), device_id_type=MESH)
                    for m, (r, n, to, ref, sem) in enumerate(messages(i, j))]

        def wait_in(ref, sem):
            pltpu.make_async_remote_copy(ref, ref, ssem.at[0, 0], sem, device_id=place.partner(), device_id_type=MESH).wait_recv()

        def hand_over(s):
            return [pltpu.make_async_remote_copy(pool.at[hand_unit(s), :, pl.ds(c * cw, cw)], dr.at[s % ndr, :, pl.ds(c * cw, cw)],
                                                 dssem.at[s % 4, c], drsem.at[s, c],
                                                 device_id=place.partner(), device_id_type=MESH) for c in range(CHUNKS)]

        def stage_a(i, j):
            u = unit(ORDER2.index((i, j)))
            msg = ORDER2.index((j, i))
            for c in hand_over(msg):
                c.wait_recv()

            @pl.loop(0, block // 32)
            def _(r):
                rows = pl.ds(pl.multiple_of(r * 32, 32), 32)
                pool[u, rows, :] = pool[u, rows, :] + dr[msg % ndr, rows, :]

            if msg + ndr < n_steps:
                pl.semaphore_signal(free.at[msg % ndr], inc=1, device_id=place.partner(), device_id_type=MESH)
            if j == 2:
                for c in copies(i, j):
                    c.start()
            if (i, j) == (0, 0):
                own_out(u).start()

        def own_out(u):
            return pltpu.make_async_copy(pool.at[u], p_ref, out_sem)

        def staged(i, j, p):
            if j == 0:
                return [pltpu.make_async_copy(m2_ref.at[i % SIDE, d], stage.at[p, d], st_sem.at[p, d]) for d in range(2)]
            d = 0 if j == 1 else 1
            return [pltpu.make_async_copy(m1_ref.at[i % SIDE, d], stage.at[p, 0, pl.ds(0, half)], st_sem.at[p, 0])]

        order = [e for s in range(n_steps + 1) for e in EVENTS2[s] + (MIDDLE2[s] if s < n_steps else [])]
        turn = {e[1:]: n % 2 for n, e in enumerate(e for e in order if e[0] == "L")}

        def load_in(i, j):
            if j == 0:
                for d in range(2):
                    wait_in(m2_ref.at[i % SIDE, d], m2sem.at[i % SIDE, d])
            else:
                d = 0 if j == 1 else 1
                wait_in(m1_ref.at[i % SIDE, d], m1sem.at[i % SIDE, d])
            for c in staged(i, j, turn[(i, j)]):
                c.start()
            if j == 0 and i in (1, -1):
                d = 0 if i == 1 else 1
                wait_in(f1.at[d], f1sem.at[d])

        def stage_b(i, j):
            p = turn[(i, j)]
            u = unit(ORDER2.index((i, j)))
            for c in staged(i, j, p):
                c.wait()
            for h in range(2):
                if (j, h) in ((1, 1), (-1, 0)):
                    continue

                @pl.loop(0, half // 16)
                def _(r, h=h):
                    rows = pl.ds(pl.multiple_of(h * half + r * 16, 16), 16)
                    near = pl.ds(pl.multiple_of(r * 16, 16), 16)
                    if j != 0:
                        pool[u, rows, :] = pool[u, rows, :] + stage[p, 0, near, :]
                    else:
                        total = pool[u, rows, :].astype(f32) + stage[p, 0, rows, :].astype(f32) + stage[p, 1, rows, :].astype(f32)
                        if (i, h) == (1, 0):
                            total = total + f1[0, near, :].astype(f32)
                        if (i, h) == (-1, 1):
                            total = total + f1[1, near, :].astype(f32)
                        pool[u, rows, :] = total.astype(bf16)
            for c in copies(i, j):
                c.start()

        def serve(events):
            for kind, i, j in events:
                if (kind, i, j) not in (("L", 0, 0), ("B", 0, 0)):
                    {"A": stage_a, "L": load_in, "B": stage_b}[kind](i, j)

        for c in step_loads(0):
            c.start()

        @pl.loop(0, n_steps)
        def _(step):
            @functools.partial(at_steps, step, n_steps)
            def _(s):
                serve(EVENTS2[s])
                if s + 1 < n_steps:
                    if s + 1 >= NS:
                        for c in copies(*ORDER2[s + 1 - NS]):
                            c.wait_send()
                    if s + 1 >= pool.shape[0] - NS:
                        for c in hand_over(s + 1 - (pool.shape[0] - NS)):
                            c.wait_send()
                    for c in step_loads(s + 1):
                        c.start()

            p = lax.rem(step, 2)
            b = place.chip(me, pick(step, [i for i, _ in ORDER2]), pick(step, [j for _, j in ORDER2]))
            scale = head ** -0.5 * LOG2E

            @pl.when(step >= 0)
            def _():
                m_sc[...] = jnp.full(m_sc.shape, NEG, f32)
                l_sc[...] = jnp.zeros(l_sc.shape, f32)
                acc_sc[...] = jnp.zeros(acc_sc.shape, f32)

            q_at = pl.ds(pl.multiple_of(b * pair, pair), pair)

            def position(at):
                return at % half + at // half % 2 * block + at // block * half

            def attend(t, width):
                size = width or KT
                rows = pl.ds(pl.multiple_of(t * KT, KT), size)
                scores = []
                for g in range(2):
                    sc = jnp.dot(kk[rows, g * 128:(g + 1) * 128], qq[g * 128:(g + 1) * 128, q_at], preferred_element_type=f32)
                    if width:
                        kp = position(lax.broadcasted_iota(jnp.int32, (pair, pair), 0))
                        qp = position(lax.broadcasted_iota(jnp.int32, (pair, pair), 1))
                        own = jnp.where(kp <= qp, sc[size - pair:], NEG)
                        sc = own if size == pair else jnp.concatenate([sc[:size - pair], own], axis=0)
                    scores.append(sc)
                for g in range(2):
                    sc = scores[g]
                    old = m_sc[g:g + 1, :]
                    top = jnp.maximum(old, jnp.max(sc, axis=0, keepdims=True))
                    keep = jnp.exp2((old - top) * scale)
                    pr = jnp.exp2((sc - top) * scale)
                    l_sc[g:g + 1, :] = l_sc[g:g + 1, :] * keep + jnp.sum(pr, axis=0, keepdims=True)
                    acc_sc[g] = acc_sc[g] * keep + jnp.dot(vv[g * head:(g + 1) * head, rows], pr.astype(bf16),
                                                           preferred_element_type=f32)
                    m_sc[g:g + 1, :] = top

            full = lax.div(b, KT // pair)

            @pl.loop(0, full)
            def _(t):
                attend(t, 0)

            for v in range(KT // pair):
                @pl.when(lax.rem(b, KT // pair) == v)
                def _(v=v):
                    attend(full, (v + 1) * pair)
                    for g in range(2):
                        o = acc_sc[g] / l_sc[g:g + 1, :]
                        lhs[p, :, pl.ds(ffl + g * head, head)] = o.T.astype(bf16)

            @functools.partial(at_steps, step, n_steps)
            def _(s):
                serve(MIDDLE2[s])
                for c in step_loads(s):
                    c.wait()

            mine, theirs = lax.rem(step, NS), NS + lax.rem(step, pool.shape[0] - NS)
            low = mine * (1 - me) + theirs * me
            high = mine * me + theirs * (1 - me)
            is_early = functools.reduce(jnp.logical_or, [step == ORDER2.index(c) for c in EARLY]) if EARLY else step < 0

            @pl.when(is_early)
            def _():
                for c in range(CHUNKS):
                    cols = slice(c * cw, (c + 1) * cw)
                    r = jnp.dot(lhs[p, :, ffl:ffl + hd2], w[ffl:ffl + hd2, cols], preferred_element_type=f32)
                    for h in range(2):
                        rows = slice(h * half, (h + 1) * half)
                        for u, first in ((low, h * block), (high, h * block + half)):
                            pool[u, rows, cols] = (pool[u, rows, cols].astype(f32) + r[first:first + half]).astype(bf16)

            @pl.when(jnp.logical_not(is_early))
            def _():
                for c in range(CHUNKS):
                    cols = slice(c * cw, (c + 1) * cw)
                    r = jnp.dot(lhs[p, :, 0:ffl + hd2], w[:, cols], preferred_element_type=f32)
                    for h in range(2):
                        rows = slice(h * half, (h + 1) * half)
                        for u, first in ((low, h * block), (high, h * block + half)):
                            pool[u, rows, cols] = r[first:first + half].astype(bf16)

            @functools.partial(at_steps, step, n_steps)
            def _(s):
                if s >= ndr:
                    pl.semaphore_wait(free.at[s % ndr], 1)
                for c in hand_over(s):
                    c.start()

        serve(EVENTS2[n_steps])
        for s in range(n_steps - NS, n_steps):
            for c in copies(*ORDER2[s]):
                c.wait_send()
        for s in range(n_steps - (pool.shape[0] - NS), n_steps):
            for c in hand_over(s):
                c.wait_send()
        own_out(unit(ORDER2.index((0, 0)))).wait()
        for d in range(2):
            wait_in(m2_ref.at[0, d], m2sem.at[0, d])
            wait_in(f2.at[d], f2sem.at[d])

    pl.run_scoped(scatter, pltpu.VMEM((NS + 3, block, width), bf16),
                  pltpu.VMEM((2, 2, block, width), bf16),
                  pltpu.SemaphoreType.DMA, pltpu.SemaphoreType.DMA((2, 4)), pltpu.SemaphoreType.DMA((2, 2)))

    for n, (_, i, j, h) in enumerate(sent):
        if (i, j) != (0, 0):
            r = rows_of(me, i, j, h)
            pltpu.make_async_remote_copy(r, r, send.at[n], recv.at[0, 0, 0], device_id=place.partner(), device_id_type=MESH).wait_send()
    for i, j in ORDER2[:-1]:
        for h in range(2):
            r = rows_of(me, i, j, h)
            pltpu.make_async_remote_copy(r, r, dsend.at[i % SIDE, j % SIDE, h], recv.at[0, 0, 0],
                                         device_id=place.partner(), device_id_type=MESH).wait_send()


def finish_kernel(x_ref, own_ref, second_ref, first_ref, y_ref):
    branch = own_ref[...].astype(f32)
    for part in (second_ref, first_ref):
        for d in range(2):
            branch = branch + part[d].astype(f32)
    y_ref[...] = (x_ref[...].astype(f32) + branch.astype(bf16).astype(f32)).astype(bf16)


def layer(x, gain, bias, w_qkv, w_up, w_down, w_out, n_tp):
    block, width = x.shape
    seq = n_tp * block
    d, groups, three, head = w_qkv.shape
    wq = w_qkv.transpose(1, 2, 3, 0).reshape(groups * three * head, d)
    ffl = w_up.shape[1]
    hd2 = groups * head
    half = block // 2
    hbm = pl.BlockSpec(memory_space=pltpu.HBM)
    V, D, S = pltpu.VMEM, pltpu.SemaphoreType.DMA, jax.ShapeDtypeStruct
    own, _, _, _, _, second, first = pl.pallas_call(
        layer_kernel,
        out_shape=(S((block, width), bf16), S((seq, width), bf16), S((seq, ffl), bf16), S((seq, width), bf16),
                   S((SIDE, 2, half, width), bf16), S((SIDE, 2, block, width), bf16), S((2, block, width), bf16)),
        in_specs=[hbm] * 7, out_specs=(hbm,) * 7,
        scratch_shapes=[
            V((ffl + hd2, width), bf16), V((groups * 128, seq), bf16), V((seq, groups * 128), bf16), V((hd2, seq), bf16),
            V((2, 2 * block, -(-(ffl + hd2) // 128) * 128), bf16), V((4, block, width), bf16),
            V((2, half, width), bf16),
            V((8, 2 * block), f32), V((8, 2 * block), f32), V((groups, head, 2 * block), f32),
            D((SIDE, SIDE, 2)), D((30,)), D((SIDE, SIDE, 2)), D((SIDE, SIDE, 2)),
            D((16, 2)), D((4, CHUNKS)), D((16, CHUNKS)), D((SIDE, 2)), D((SIDE, 2)), D((2,)), D((2,)),
            pltpu.SemaphoreType.REGULAR((4,)), D((2,))],
        compiler_params=pltpu.CompilerParams(collective_id=0, has_side_effects=True, vmem_limit_bytes=67043328),
        name="parallel_layer",
    )(x, gain.reshape(1, -1), bias.reshape(1, -1), wq, w_up, w_down, w_out)
    rows = block // FINAL_STEPS
    flat = pl.BlockSpec((rows, width), lambda n: (n, 0))
    return pl.pallas_call(
        finish_kernel,
        out_shape=S((block, width), bf16),
        grid=(FINAL_STEPS,),
        in_specs=[flat, flat, pl.BlockSpec((None, 2, rows, width), lambda n: (0, 0, n, 0)),
                  pl.BlockSpec((2, rows, width), lambda n: (0, n, 0))],
        out_specs=flat,
        name="finish",
    )(x, own, second, first)


def solution(mesh):
    n_tp = mesh.shape["tp"]
    assert n_tp == 2 * SIDE * SIDE

    def local_layer(x_blk, ln_gain, ln_bias, w_qkv, w_out, w_up, w_down):
        x = x_blk.reshape(x_blk.shape[1:])
        return layer(x, ln_gain, ln_bias, w_qkv, w_up, w_down, w_out, n_tp)[None]

    return jax.shard_map(
        local_layer, mesh=mesh,
        in_specs=(P("dp", "tp", None), P(), P(), P(None, "tp", None, None),
                  P("tp", None), P(None, "tp"), P("tp", None)),
        out_specs=P("dp", "tp", None), check_vma=False)
```

```python
import functools

import jax
import jax.numpy as jnp
from jax import lax
from jax.experimental import pallas as pl
from jax.experimental.pallas import tpu as pltpu
from jax.sharding import PartitionSpec as P

OFFSETS = {"o": 0, "p": 1, "m": -1, "t": 2}


def place_of(text):
    return OFFSETS[text[0]], OFFSETS[text[1]]


def split(text, size):
    return [text[n:n + size] for n in range(0, len(text), size)]


def gather_events(text):
    return [("l", int(e[1:3])) if e[0] == "l" else (e[0],) + place_of(e[1:]) + (int(e[3]),) for e in split(text, 4)]


def scatter_events(text):
    return [(e[0],) + place_of(e[1:]) for e in split(text, 3)]


TILES = [
    "oo0oo1",
    "op0om1",
    "po0mo1",
    "op1om0",
    "po1mo0",
    "pp0mm1",
    "ot0ot1",
    "to0to1",
    "pm1mp0",
    "pm0mp1",
    "pt0mt1",
    "tp0tm1",
    "pt1mt0",
    "tp1tm0",
    "tt0tt1",
    "pp1mm0",
]
TILES = [[(place_of(u), int(u[2])) for u in split(text, 3)] for text in TILES]
BEFORE = [
    "aoo0aoo1Eoo1Eoo0Woo0Woo1Uoo1Uoo0Doo0Doo1l00-",
    "aop0aom1apo0amo1Emo1Wpo0Umo1Uom1Dpo0Dop0l01-l02-",
    "",
    "Upo0Dmo1aop1aom0apo1amo0l03-l04-",
    "",
    "Upo1Dmo0app0amm1ato0ato1l05-",
    "aot0aot1Uto1Dto0l06-",
    "apm0amp1",
    "apm1amp0l08-",
    "Upm1Dmp0l09-atp0atm1",
    "Utm1Dtp0apt0amt1l10-",
    "atp1atm0",
    "apt1amt0l12-",
    "att0att1",
    "app1amm0",
    "",
]
BEFORE = [gather_events(text) for text in BEFORE]
BETWEEN = [
    "",
    "",
    "",
    "",
    "",
    "",
    "Umm1Dpp0l07-",
    "Uto0Dto1",
    "",
    "",
    "Umo0Dpo1l11-",
    "",
    "l13-",
    "l14-",
    "l15-",
    "",
]
BETWEEN = [gather_events(text) for text in BETWEEN]
DOWNS = [0, 6, 7, 10, 11, 12, 13, 14]
EARLY = [place_of(text) for text in split("oootptmttotptmtt", 2)]
ORDER2 = [place_of(text) for text in split("tttppttmmtppmmpmmpottopoopmoomoo", 2)]
EVENTS2 = [
    "",
    "",
    "",
    "Apt",
    "Ltp",
    "Amt",
    "Btm",
    "Bpp",
    "Bmm",
    "AmpLmp",
    "Bpm",
    "AtoLto",
    "",
    "Aop",
    "",
    "Aom",
    "BpoBmoAooLomLopBomBopLooBoo",
]
EVENTS2 = [scatter_events(text) for text in EVENTS2]
MIDDLE2 = [
    "",
    "Att",
    "",
    "Atp",
    "Btp",
    "AtmLtm",
    "AppLpp",
    "AmmLmm",
    "",
    "BmpApmLpm",
    "",
    "BtoAot",
    "",
    "Apo",
    "",
    "LpoAmoLmo",
]
MIDDLE2 = [scatter_events(text) for text in MIDDLE2]
NS = 11
MESH = pl.DeviceIdType.MESH
SIDE = 4
LN_EPS = 1e-5
f32, bf16 = jnp.float32, jnp.bfloat16
KT = 1024
CHUNKS = 3
FINAL_STEPS = 2
NEG = -1e30
LOG2E = 1.4426950408889634


class Place:
    def __init__(self):
        self.tp = lax.axis_index("tp")
        self.colour = lax.rem(self.tp, 2)
        chip = lax.div(self.tp, 2)
        self.x, self.y = lax.rem(chip, SIDE), lax.div(chip, SIDE)

    def chip(self, colour, i, j):
        dx = (1 - colour) * i + colour * j
        dy = (1 - colour) * j + colour * i
        return lax.rem(self.y + dy + SIDE, SIDE) * SIDE + lax.rem(self.x + dx + SIDE, SIDE)

    def device(self, i, j):
        return {"tp": self.chip(self.colour, i, j) * 2 + self.colour}

    def partner(self):
        return {"tp": self.tp + 1 - 2 * self.colour}


def greet(place):
    barrier = pltpu.get_barrier_semaphore()
    others = [place.device(1, 0), place.device(-1, 0), place.device(0, 1), place.device(0, -1), place.partner()]
    for other in others:
        pl.semaphore_signal(barrier, inc=1, device_id=other, device_id_type=MESH)
    return lambda: pl.semaphore_wait(barrier, len(others))


ROUTES = {"W": (-1, 0), "E": (1, 0), "D": (0, -1), "U": (0, 1)}


def at_steps(step, count, body):
    for first in range(0, count, 4):
        @pl.when(jnp.logical_and(step >= first, step < first + 4))
        def _(first=first):
            for s in range(first, min(first + 4, count)):
                @pl.when(step == s)
                def _(s=s):
                    body(s)


def pick(step, values):
    r = jnp.int32(values[0])
    for n, v in enumerate(values[1:], 1):
        r = jnp.where(step == n, jnp.int32(v), r)
    return r


def layer_kernel(x_ref, gain_ref, bias_ref, wqkv_ref, wup_ref, wdown_ref, wout_ref,
                 p_ref, full_ref, act_ref, m_ref, m1_ref, m2_ref, f2,
                 w, qq, kk, vv, lhs, dr, f1, m_sc, l_sc, acc_sc,
                 recv, send, drecv, dsend, ssem, dssem, drsem, m1sem, m2sem, f1sem, f2sem, free, w_sem):
    place = Place()
    me = place.colour
    block, width = x_ref.shape
    half = block // 2
    ffl = wup_ref.shape[1]
    hd2 = wout_ref.shape[0]
    head = hd2 // 2
    pair = 2 * block
    n_steps = len(TILES)
    ndr = dr.shape[0]
    cw = width // CHUNKS

    wloads = [pltpu.make_async_copy(wdown_ref, w.at[pl.ds(0, ffl)], w_sem.at[0]),
              pltpu.make_async_copy(wout_ref, w.at[pl.ds(ffl, hd2)], w_sem.at[1])]

    def rows_of(colour, i, j, h):
        first = (place.chip(colour, i, j) * 2 + colour) * block + h * half
        return full_ref.at[pl.ds(pl.multiple_of(first, half), half)]

    def chip_rows(ref, i, j):
        return ref.at[pl.ds(pl.multiple_of(place.chip(me, i, j) * pair, pair), pair)]

    sent = [e for t in range(n_steps) for e in BEFORE[t] + BETWEEN[t] if e[0] in ROUTES]

    def stored(unit):
        (i, j), h = unit
        return pl.ds(pl.multiple_of(place.chip(me, i, j) * pair + h * block, block), block)

    def gather(xs, own, gain, bias, wqkv, wup, tile, acts, mst, in_sem, pw_sem, tile_sem, out_sem, mst_sem):
        loads = [pltpu.make_async_copy(x_ref, xs, in_sem.at[0]),
                 pltpu.make_async_copy(gain_ref, gain, in_sem.at[1]),
                 pltpu.make_async_copy(bias_ref, bias, in_sem.at[2])]
        pwloads = [pltpu.make_async_copy(wqkv_ref, wqkv, pw_sem.at[0]), pltpu.make_async_copy(wup_ref, wup, pw_sem.at[1])]
        for c in loads + pwloads + wloads:
            c.start()
        met = greet(place)
        for c in loads:
            c.wait()

        def norm_rows(start):
            g = gain[...]
            b = bias[...]

            @pl.loop(0, half // 16)
            def _(r):
                rows = pl.ds(pl.multiple_of(start + r * 16, 16), 16)
                v = xs[rows, :].astype(f32)
                mean = jnp.mean(v, axis=-1, keepdims=True)
                cen = v - mean
                var = jnp.mean(cen * cen, axis=-1, keepdims=True)
                own[rows, :] = (cen * lax.rsqrt(var + LN_EPS) * g + b).astype(bf16)

        def source(i, j, h):
            return own.at[pl.ds(h * half, half)] if (i, j) == (0, 0) else rows_of(me, i, j, h)

        def forward(kind, i, j, h):
            di, dj = ROUTES[kind]
            ri, rj = (i - di) % SIDE, (j - dj) % SIDE
            pltpu.make_async_remote_copy(source(i, j, h), rows_of(me, i, j, h), send.at[sent.index((kind, i, j, h))],
                                         recv.at[ri, rj, h], device_id=place.device(di, dj), device_id_type=MESH).start()

        def wait_block(colour, i, j, h, sem):
            r = rows_of(colour, i, j, h)
            pltpu.make_async_remote_copy(r, r, send.at[0], sem.at[i % SIDE, j % SIDE, h],
                                         device_id=place.partner(), device_id_type=MESH).wait_recv()

        def arrived(i, j, h):
            if (i, j) != (0, 0):
                wait_block(me, i, j, h, recv)
            pltpu.make_async_remote_copy(source(i, j, h), rows_of(me, i, j, h), dsend.at[i % SIDE, j % SIDE, h],
                                         drecv.at[i % SIDE, j % SIDE, h], device_id=place.partner(), device_id_type=MESH).start()

        def tile_parts(t, load):
            parts = []
            for u, ((i, j), h) in enumerate(TILES[t]):
                for n, colour in enumerate((me, 1 - me)):
                    if (i, j) == (0, 0) and n == 0:
                        if load:
                            tile[t % 2, pl.ds(pl.multiple_of(u * block + colour * half, half), half), :] = own[pl.ds(h * half, half), :]
                        continue
                    if load and n == 1:
                        wait_block(colour, j, i, h, drecv)
                    src = rows_of(me, i, j, h) if n == 0 else rows_of(colour, j, i, h)
                    parts.append(pltpu.make_async_copy(
                        src, tile.at[t % 2, pl.ds(pl.multiple_of(u * block + colour * half, half), half)],
                        tile_sem.at[t % 2, 2 * u + n]))
            return parts

        def act_out(t):
            return [pltpu.make_async_copy(acts.at[t % 2, pl.ds(u * block, block)], act_ref.at[stored(unit)], out_sem.at[t % 2, u])
                    for u, unit in enumerate(TILES[t]) if unit[0] not in EARLY]

        def m_out(t):
            return [pltpu.make_async_copy(mst.at[c, pl.ds(u * block, block)],
                                          m_ref.at[stored(unit), pl.ds(c * cw, cw)], mst_sem.at[c, u])
                    for c in range(CHUNKS) for u, unit in enumerate(TILES[t]) if unit[0] in EARLY]

        def serve(events):
            for e in events:
                if e[0] == "a":
                    arrived(*e[1:])
                elif e[0] == "l":
                    for c in tile_parts(e[1], True):
                        c.start()
                else:
                    forward(*e)

        norm_rows(0)
        norm_rows(half)
        met()
        serve([e for e in BEFORE[0] if e[0] != "l"])
        for g in range(2):
            qq[pl.ds(g * 128 + head, 128 - head), :] = jnp.zeros((128 - head, qq.shape[1]), bf16)

        @pl.loop(0, n_steps)
        def _(step):
            @functools.partial(at_steps, step, n_steps)
            def _(s):
                serve([e for e in BEFORE[s] if s or e[0] == "l"])
                if s >= 2:
                    for c in act_out(s - 2):
                        c.wait()
                if s == 0:
                    for c in pwloads:
                        c.wait()
                for c in tile_parts(s, False):
                    c.wait()

            p = lax.rem(step, 2)
            homes = []
            for u in range(2):
                units = [t[u] for t in TILES]
                b = place.chip(me, pick(step, [i for (i, _), _ in units]), pick(step, [j for (_, j), _ in units]))
                homes.append(pl.ds(pl.multiple_of(b * pair + pick(step, [h for _, h in units]) * block, block), block))

            @pl.when(step >= 0)
            def _():
                n = tile[p]
                qkv = lax.dot_general(wqkv[...], n, (((1,), (1,)), ((), ())), preferred_element_type=f32)
                for g in range(2):
                    base = g * 3 * head
                    keys = qkv[base + head:base + 2 * head]
                    keys = jnp.concatenate([keys, jnp.zeros((128 - head, pair), f32)], axis=0).T.astype(bf16)
                    for u in range(2):
                        cols = slice(u * block, (u + 1) * block)
                        qq[pl.ds(g * 128, head), homes[u]] = qkv[base:base + head, cols].astype(bf16)
                        kk[homes[u], pl.ds(g * 128, 128)] = keys[cols]
                        vv[pl.ds(g * head, head), homes[u]] = qkv[base + 2 * head:base + 3 * head, cols].astype(bf16)
                hid = jnp.dot(n, wup[...], preferred_element_type=f32)
                acts[p] = (0.5 * hid * (1.0 + lax.erf(hid * (0.5 ** 0.5)))).astype(bf16)

            @functools.partial(at_steps, step, n_steps)
            def _(s):
                serve(BETWEEN[s])
                for c in act_out(s):
                    c.start()
                if s in DOWNS:
                    if s == DOWNS[0]:
                        for c in wloads:
                            c.wait()
                    else:
                        for c in m_out(DOWNS[DOWNS.index(s) - 1]):
                            c.wait()

            @pl.when(functools.reduce(jnp.logical_or, [step == s for s in DOWNS]))
            def _():
                for c in range(CHUNKS):
                    mst[c] = jnp.dot(acts[p], w[0:ffl, c * cw:(c + 1) * cw], preferred_element_type=f32).astype(bf16)

            @functools.partial(at_steps, step, n_steps)
            def _(s):
                if s in DOWNS:
                    for c in m_out(s):
                        c.start()

        for s in (n_steps - 2, n_steps - 1):
            for c in act_out(s):
                c.wait()
        for c in m_out(DOWNS[-1]):
            c.wait()
        for n, (_, i, j, h) in enumerate(sent):
            if (i, j) == (0, 0):
                pltpu.make_async_remote_copy(source(0, 0, h), rows_of(me, 0, 0, h), send.at[n], recv.at[0, 0, 0],
                                             device_id=place.partner(), device_id_type=MESH).wait_send()
        for h in range(2):
            pltpu.make_async_remote_copy(source(0, 0, h), rows_of(me, 0, 0, h), dsend.at[0, 0, h], recv.at[0, 0, 0],
                                         device_id=place.partner(), device_id_type=MESH).wait_send()

    pl.run_scoped(
        gather, pltpu.VMEM((block, width), bf16), pltpu.VMEM((block, width), bf16), pltpu.VMEM((1, width), f32), pltpu.VMEM((1, width), f32),
        pltpu.VMEM(wqkv_ref.shape, bf16), pltpu.VMEM(wup_ref.shape, bf16), pltpu.VMEM((2, pair, width), bf16),
        pltpu.VMEM((2, pair, ffl), bf16), pltpu.VMEM((CHUNKS, pair, cw), bf16),
        pltpu.SemaphoreType.DMA((3,)), pltpu.SemaphoreType.DMA((2,)), pltpu.SemaphoreType.DMA((2, 4)), pltpu.SemaphoreType.DMA((2, 2)),
        pltpu.SemaphoreType.DMA((CHUNKS, 2)))

    def scatter(pool, stage, out_sem, lq_sem, st_sem):

        def unit(s):
            return s % NS

        def hand_unit(s):
            return NS + s % (pool.shape[0] - NS)

        def step_loads(s):
            i, j = ORDER2[s]
            base = place.chip(me, i, j) * pair
            if (i, j) in EARLY:
                res = []
                for n, (colour, u) in enumerate(((me, unit(s)), (1 - me, hand_unit(s)))):
                    for h in range(2):
                        at = pl.ds(pl.multiple_of(base + h * block + colour * half, half), half)
                        res.append(pltpu.make_async_copy(m_ref.at[at], pool.at[u, pl.ds(h * half, half)], lq_sem.at[s % 2, 2 * n + h]))
                return res
            return [pltpu.make_async_copy(chip_rows(act_ref, i, j), lhs.at[s % 2, :, pl.ds(0, ffl)], lq_sem.at[s % 2, 0])]

        def messages(i, j):
            if j == 2:
                return [(0, half, (0, 1), m1_ref.at[i % SIDE, 0], m1sem.at[i % SIDE, 0]),
                        (half, half, (0, -1), m1_ref.at[i % SIDE, 1], m1sem.at[i % SIDE, 1])]
            if j == 1:
                return [(0, block, (0, 1), m2_ref.at[i % SIDE, 0], m2sem.at[i % SIDE, 0])]
            if j == -1:
                return [(0, block, (0, -1), m2_ref.at[i % SIDE, 1], m2sem.at[i % SIDE, 1])]
            if i == 2:
                return [(0, half, (1, 0), f1.at[0], f1sem.at[0]), (half, half, (-1, 0), f1.at[1], f1sem.at[1])]
            if i == 1:
                return [(0, block, (1, 0), f2.at[0], f2sem.at[0])]
            if i == -1:
                return [(0, block, (-1, 0), f2.at[1], f2sem.at[1])]
            return []

        def copies(i, j):
            s = ORDER2.index((i, j))
            return [pltpu.make_async_remote_copy(pool.at[unit(s), pl.ds(r, n)], ref, ssem.at[s, m], sem,
                                                 device_id=place.device(*to), device_id_type=MESH)
                    for m, (r, n, to, ref, sem) in enumerate(messages(i, j))]

        def wait_in(ref, sem):
            pltpu.make_async_remote_copy(ref, ref, ssem.at[0, 0], sem, device_id=place.partner(), device_id_type=MESH).wait_recv()

        def hand_over(s):
            return [pltpu.make_async_remote_copy(pool.at[hand_unit(s), :, pl.ds(c * cw, cw)], dr.at[s % ndr, :, pl.ds(c * cw, cw)],
                                                 dssem.at[s % 4, c], drsem.at[s, c],
                                                 device_id=place.partner(), device_id_type=MESH) for c in range(CHUNKS)]

        def stage_a(i, j):
            u = unit(ORDER2.index((i, j)))
            msg = ORDER2.index((j, i))
            for c in hand_over(msg):
                c.wait_recv()

            @pl.loop(0, block // 32)
            def _(r):
                rows = pl.ds(pl.multiple_of(r * 32, 32), 32)
                pool[u, rows, :] = pool[u, rows, :] + dr[msg % ndr, rows, :]

            if msg + ndr < n_steps:
                pl.semaphore_signal(free.at[msg % ndr], inc=1, device_id=place.partner(), device_id_type=MESH)
            if j == 2:
                for c in copies(i, j):
                    c.start()
            if (i, j) == (0, 0):
                own_out(u).start()

        def own_out(u):
            return pltpu.make_async_copy(pool.at[u], p_ref, out_sem)

        def staged(i, j, p):
            if j == 0:
                return [pltpu.make_async_copy(m2_ref.at[i % SIDE, d], stage.at[p, d], st_sem.at[p, d]) for d in range(2)]
            d = 0 if j == 1 else 1
            return [pltpu.make_async_copy(m1_ref.at[i % SIDE, d], stage.at[p, 0, pl.ds(0, half)], st_sem.at[p, 0])]

        order = [e for s in range(n_steps + 1) for e in EVENTS2[s] + (MIDDLE2[s] if s < n_steps else [])]
        turn = {e[1:]: n % 2 for n, e in enumerate(e for e in order if e[0] == "L")}

        def load_in(i, j):
            if j == 0:
                for d in range(2):
                    wait_in(m2_ref.at[i % SIDE, d], m2sem.at[i % SIDE, d])
            else:
                d = 0 if j == 1 else 1
                wait_in(m1_ref.at[i % SIDE, d], m1sem.at[i % SIDE, d])
            for c in staged(i, j, turn[(i, j)]):
                c.start()
            if j == 0 and i in (1, -1):
                d = 0 if i == 1 else 1
                wait_in(f1.at[d], f1sem.at[d])

        def stage_b(i, j):
            p = turn[(i, j)]
            u = unit(ORDER2.index((i, j)))
            for c in staged(i, j, p):
                c.wait()
            for h in range(2):
                if (j, h) in ((1, 1), (-1, 0)):
                    continue

                @pl.loop(0, half // 16)
                def _(r, h=h):
                    rows = pl.ds(pl.multiple_of(h * half + r * 16, 16), 16)
                    near = pl.ds(pl.multiple_of(r * 16, 16), 16)
                    if j != 0:
                        pool[u, rows, :] = pool[u, rows, :] + stage[p, 0, near, :]
                    else:
                        total = pool[u, rows, :].astype(f32) + stage[p, 0, rows, :].astype(f32) + stage[p, 1, rows, :].astype(f32)
                        if (i, h) == (1, 0):
                            total = total + f1[0, near, :].astype(f32)
                        if (i, h) == (-1, 1):
                            total = total + f1[1, near, :].astype(f32)
                        pool[u, rows, :] = total.astype(bf16)
            for c in copies(i, j):
                c.start()

        def serve(events):
            for kind, i, j in events:
                if (kind, i, j) not in (("L", 0, 0), ("B", 0, 0)):
                    {"A": stage_a, "L": load_in, "B": stage_b}[kind](i, j)

        for c in step_loads(0):
            c.start()

        @pl.loop(0, n_steps)
        def _(step):
            @functools.partial(at_steps, step, n_steps)
            def _(s):
                serve(EVENTS2[s])
                if s + 1 < n_steps:
                    if s + 1 >= NS:
                        for c in copies(*ORDER2[s + 1 - NS]):
                            c.wait_send()
                    if s + 1 >= pool.shape[0] - NS:
                        for c in hand_over(s + 1 - (pool.shape[0] - NS)):
                            c.wait_send()
                    for c in step_loads(s + 1):
                        c.start()

            p = lax.rem(step, 2)
            b = place.chip(me, pick(step, [i for i, _ in ORDER2]), pick(step, [j for _, j in ORDER2]))
            scale = head ** -0.5 * LOG2E

            @pl.when(step >= 0)
            def _():
                m_sc[...] = jnp.full(m_sc.shape, NEG, f32)
                l_sc[...] = jnp.zeros(l_sc.shape, f32)
                acc_sc[...] = jnp.zeros(acc_sc.shape, f32)

            q_at = pl.ds(pl.multiple_of(b * pair, pair), pair)

            def position(at):
                return at % half + at // half % 2 * block + at // block * half

            def attend(t, width):
                size = width or KT
                rows = pl.ds(pl.multiple_of(t * KT, KT), size)
                scores = []
                for g in range(2):
                    sc = jnp.dot(kk[rows, g * 128:(g + 1) * 128], qq[g * 128:(g + 1) * 128, q_at], preferred_element_type=f32)
                    if width:
                        kp = position(lax.broadcasted_iota(jnp.int32, (pair, pair), 0))
                        qp = position(lax.broadcasted_iota(jnp.int32, (pair, pair), 1))
                        own = jnp.where(kp <= qp, sc[size - pair:], NEG)
                        sc = own if size == pair else jnp.concatenate([sc[:size - pair], own], axis=0)
                    scores.append(sc)
                for g in range(2):
                    sc = scores[g]
                    old = m_sc[g:g + 1, :]
                    top = jnp.maximum(old, jnp.max(sc, axis=0, keepdims=True))
                    keep = jnp.exp2((old - top) * scale)
                    pr = jnp.exp2((sc - top) * scale)
                    l_sc[g:g + 1, :] = l_sc[g:g + 1, :] * keep + jnp.sum(pr, axis=0, keepdims=True)
                    acc_sc[g] = acc_sc[g] * keep + jnp.dot(vv[g * head:(g + 1) * head, rows], pr.astype(bf16),
                                                           preferred_element_type=f32)
                    m_sc[g:g + 1, :] = top

            full = lax.div(b, KT // pair)

            @pl.loop(0, full)
            def _(t):
                attend(t, 0)

            for v in range(KT // pair):
                @pl.when(lax.rem(b, KT // pair) == v)
                def _(v=v):
                    attend(full, (v + 1) * pair)
                    for g in range(2):
                        o = acc_sc[g] / l_sc[g:g + 1, :]
                        lhs[p, :, pl.ds(ffl + g * head, head)] = o.T.astype(bf16)

            @functools.partial(at_steps, step, n_steps)
            def _(s):
                serve(MIDDLE2[s])
                for c in step_loads(s):
                    c.wait()

            mine, theirs = lax.rem(step, NS), NS + lax.rem(step, pool.shape[0] - NS)
            low = mine * (1 - me) + theirs * me
            high = mine * me + theirs * (1 - me)
            is_early = functools.reduce(jnp.logical_or, [step == ORDER2.index(c) for c in EARLY]) if EARLY else step < 0

            @pl.when(is_early)
            def _():
                for c in range(CHUNKS):
                    cols = slice(c * cw, (c + 1) * cw)
                    r = jnp.dot(lhs[p, :, ffl:ffl + hd2], w[ffl:ffl + hd2, cols], preferred_element_type=f32)
                    for h in range(2):
                        rows = slice(h * half, (h + 1) * half)
                        for u, first in ((low, h * block), (high, h * block + half)):
                            pool[u, rows, cols] = (pool[u, rows, cols].astype(f32) + r[first:first + half]).astype(bf16)

            @pl.when(jnp.logical_not(is_early))
            def _():
                for c in range(CHUNKS):
                    cols = slice(c * cw, (c + 1) * cw)
                    r = jnp.dot(lhs[p, :, 0:ffl + hd2], w[:, cols], preferred_element_type=f32)
                    for h in range(2):
                        rows = slice(h * half, (h + 1) * half)
                        for u, first in ((low, h * block), (high, h * block + half)):
                            pool[u, rows, cols] = r[first:first + half].astype(bf16)

            @functools.partial(at_steps, step, n_steps)
            def _(s):
                if s >= ndr:
                    pl.semaphore_wait(free.at[s % ndr], 1)
                for c in hand_over(s):
                    c.start()

        serve(EVENTS2[n_steps])
        for s in range(n_steps - NS, n_steps):
            for c in copies(*ORDER2[s]):
                c.wait_send()
        for s in range(n_steps - (pool.shape[0] - NS), n_steps):
            for c in hand_over(s):
                c.wait_send()
        own_out(unit(ORDER2.index((0, 0)))).wait()
        for d in range(2):
            wait_in(m2_ref.at[0, d], m2sem.at[0, d])
            wait_in(f2.at[d], f2sem.at[d])

    pl.run_scoped(scatter, pltpu.VMEM((NS + 3, block, width), bf16),
                  pltpu.VMEM((2, 2, block, width), bf16),
                  pltpu.SemaphoreType.DMA, pltpu.SemaphoreType.DMA((2, 4)), pltpu.SemaphoreType.DMA((2, 2)))

    for n, (_, i, j, h) in enumerate(sent):
        if (i, j) != (0, 0):
            r = rows_of(me, i, j, h)
            pltpu.make_async_remote_copy(r, r, send.at[n], recv.at[0, 0, 0], device_id=place.partner(), device_id_type=MESH).wait_send()
    for i, j in ORDER2[:-1]:
        for h in range(2):
            r = rows_of(me, i, j, h)
            pltpu.make_async_remote_copy(r, r, dsend.at[i % SIDE, j % SIDE, h], recv.at[0, 0, 0],
                                         device_id=place.partner(), device_id_type=MESH).wait_send()


def finish_kernel(x_ref, own_ref, second_ref, first_ref, y_ref):
    branch = own_ref[...].astype(f32)
    for part in (second_ref, first_ref):
        for d in range(2):
            branch = branch + part[d].astype(f32)
    y_ref[...] = (x_ref[...].astype(f32) + branch.astype(bf16).astype(f32)).astype(bf16)


def layer(x, gain, bias, w_qkv, w_up, w_down, w_out, n_tp):
    block, width = x.shape
    seq = n_tp * block
    d, groups, three, head = w_qkv.shape
    wq = w_qkv.transpose(1, 2, 3, 0).reshape(groups * three * head, d)
    ffl = w_up.shape[1]
    hd2 = groups * head
    half = block // 2
    hbm = pl.BlockSpec(memory_space=pltpu.HBM)
    V, D, S = pltpu.VMEM, pltpu.SemaphoreType.DMA, jax.ShapeDtypeStruct
    own, _, _, _, _, second, first = pl.pallas_call(
        layer_kernel,
        out_shape=(S((block, width), bf16), S((seq, width), bf16), S((seq, ffl), bf16), S((seq, width), bf16),
                   S((SIDE, 2, half, width), bf16), S((SIDE, 2, block, width), bf16), S((2, block, width), bf16)),
        in_specs=[hbm] * 7, out_specs=(hbm,) * 7,
        scratch_shapes=[
            V((ffl + hd2, width), bf16), V((groups * 128, seq), bf16), V((seq, groups * 128), bf16), V((hd2, seq), bf16),
            V((2, 2 * block, -(-(ffl + hd2) // 128) * 128), bf16), V((4, block, width), bf16),
            V((2, half, width), bf16),
            V((8, 2 * block), f32), V((8, 2 * block), f32), V((groups, head, 2 * block), f32),
            D((SIDE, SIDE, 2)), D((30,)), D((SIDE, SIDE, 2)), D((SIDE, SIDE, 2)),
            D((16, 2)), D((4, CHUNKS)), D((16, CHUNKS)), D((SIDE, 2)), D((SIDE, 2)), D((2,)), D((2,)),
            pltpu.SemaphoreType.REGULAR((4,)), D((2,))],
        compiler_params=pltpu.CompilerParams(collective_id=0, has_side_effects=True, vmem_limit_bytes=67043328),
        name="parallel_layer",
    )(x, gain.reshape(1, -1), bias.reshape(1, -1), wq, w_up, w_down, w_out)
    rows = block // FINAL_STEPS
    flat = pl.BlockSpec((rows, width), lambda n: (n, 0))
    return pl.pallas_call(
        finish_kernel,
        out_shape=S((block, width), bf16),
        grid=(FINAL_STEPS,),
        in_specs=[flat, flat, pl.BlockSpec((None, 2, rows, width), lambda n: (0, 0, n, 0)),
                  pl.BlockSpec((2, rows, width), lambda n: (0, n, 0))],
        out_specs=flat,
        name="finish",
    )(x, own, second, first)


def solution(mesh):
    n_tp = mesh.shape["tp"]
    assert n_tp == 2 * SIDE * SIDE

    def local_layer(x_blk, ln_gain, ln_bias, w_qkv, w_out, w_up, w_down):
        x = x_blk.reshape(x_blk.shape[1:])
        return layer(x, ln_gain, ln_bias, w_qkv, w_up, w_down, w_out, n_tp)[None]

    return jax.shard_map(
        local_layer, mesh=mesh,
        in_specs=(P("dp", "tp", None), P(), P(), P(None, "tp", None, None),
                  P("tp", None), P(None, "tp"), P("tp", None)),
        out_specs=P("dp", "tp", None), check_vma=False)
```
